128 devices in a mesh: col: 32 (over y, z, core), grp: 4 (over x).
Axes of the slice: x: 4, y: 4, z: 4, core: 2. Of those that a mesh axis runs over, the one named last changes fastest.
Arguments:
- density_now: float32 [2, 32768, 768], P(None, ('col', 'grp')), may hold values from -6 to 6
- density_before: float32 [2, 32768, 768], P(None, ('col', 'grp')), may hold values from -6 to 6
- source: float32 [2, 32768, 768], P(None, ('col', 'grp')), may hold values from -8 to 8
- response: float32 [32768, 768], P(('col', 'grp')), may hold values from 0.5 to 4
- history_density: bfloat16 [7, 2, 32768, 768], P(None, None, ('col', 'grp')), may hold values from -6 to 6
- history_residual: bfloat16 [7, 2, 32768, 768], P(None, None, ('col', 'grp')), may hold values from -6 to 6
- column_shell: int32 [32768], P(('col', 'grp')), may hold values from 1 to 131072, as said below
- screening: float32 [1], replicated, may hold values from 1466 to 36672
Outputs:
- slab_density: float32 [2, 2, 768, 32768], P(None, None, 'col', 'grp')
- mixed_density: float32 [2, 32768, 768], P(None, ('col', 'grp'))
- residual_norm: float32 [2], replicated
The draws below stay inside these ranges and needn't reach their ends.
Inputs may be any that keep to these rules, and one draw needn't show every extreme that they name: `column_shell`: column j's value lies between 1 + j * s and (j + 1) * s, where s = (383^2 - 1) // 32768.
All inputs are finite; a program needn't handle non-finite values.
Results may differ from the reference program's by a relative error of at most 0.0038.
Values sent between devices are 32-bit elements; how exact they have to be, the bound alone decides.
A program may use at most 192 MiB of HBM per device.

```python
import math
import jax
import jax.numpy as jnp
from jax import lax

NZ = 768
COL_DEV = 256
HIST = 8
ITERS = 2
COLS = 32768
CUT2 = 146689
N_COL = 32
N_GRP = 4


def normal_part(key, tag, shape):
    return jax.random.truncated_normal(jax.random.fold_in(key, tag), -4.0, 4.0, shape, jnp.float32)


def response_field(key):
    return jnp.exp(jax.random.uniform(jax.random.fold_in(key, 1), (COLS, NZ), jnp.float32, math.log(0.5), math.log(4.0)))


def history_coefficients(key):
    return jax.random.uniform(jax.random.fold_in(key, 2), (HIST - 1,), jnp.float32, -1.0, 1.0)


def step_entry(key, position):
    summed = 0.6 * normal_part(jax.random.fold_in(key, 3), position, (2, COLS, NZ))
    return summed


def fixed_point(key):
    return normal_part(key, 6, (2, COLS, NZ))


def current_density(key):
    coeffs = history_coefficients(key)
    summed = fixed_point(key) + 0.3 * normal_part(key, 7, (2, COLS, NZ))
    for position in range(HIST - 1):
        summed = summed + coeffs[position] * step_entry(key, position)
    return jnp.clip(summed, -6.0, 6.0)


def draw_density_now(key, part):
    return current_density(key)


def draw_density_before(key, part):
    summed = current_density(key) + 0.5 * normal_part(key, 8, (2, COLS, NZ))
    return jnp.clip(summed, -6.0, 6.0)


def draw_source(key, part):
    return jnp.clip(response_field(key)[None] * fixed_point(key), -8.0, 8.0)


def draw_response(key, part):
    return response_field(key)


def draw_history_density(key, part):
    entries = [step_entry(key, position) for position in range(HIST - 1)]
    return jnp.clip(jnp.stack(entries), -6.0, 6.0).astype(jnp.bfloat16)


def draw_history_residual(key, part):
    stiffness = response_field(key)
    entries = []
    for position in range(HIST - 1):
        noise = 0.3 * normal_part(jax.random.fold_in(key, 5), position, (2, COLS, NZ))
        entries.append(noise - stiffness[None] * step_entry(key, position))
    return jnp.clip(jnp.stack(entries), -6.0, 6.0).astype(jnp.bfloat16)


def draw_column_shell(key, part):
    radius_squared = (NZ // 2 - 1) ** 2
    spacing = (radius_squared - 1) // COLS
    lowest = 1 + jnp.arange(COLS, dtype=jnp.int32) * spacing
    return lowest + jax.random.randint(jax.random.fold_in(key, 9), (COLS,), 0, spacing, jnp.int32)


def setup_inputs(seed: int = 0) -> dict:
    keys = jax.random.split(jax.random.key(seed), 9)
    return {
        "density_now": draw_density_now(jax.random.fold_in(keys[8], 71), 0),
        "density_before": draw_density_before(jax.random.fold_in(keys[8], 71), 0),
        "source": draw_source(jax.random.fold_in(keys[8], 71), 0),
        "response": draw_response(jax.random.fold_in(keys[8], 71), 0),
        "history_density": draw_history_density(jax.random.fold_in(keys[8], 71), 0),
        "history_residual": draw_history_residual(jax.random.fold_in(keys[8], 71), 0),
        "column_shell": draw_column_shell(jax.random.fold_in(keys[8], 71), 0),
        "screening": jnp.clip(jnp.exp(jax.random.uniform(keys[7], (1,), jnp.float32, math.log(1466.0), math.log(36672.0))), 1466.0, 36672.0),
    }


MIXING = 0.7

def rounded(values):
    return lax.optimization_barrier(values.astype(jnp.bfloat16)).astype(jnp.float32)

def reference(density_now, density_before, source, response, history_density, history_residual, column_shell, screening):
    midpoint = NZ // 2
    slot_index = jnp.arange(NZ, dtype=jnp.int32)
    signed = jnp.where(slot_index < midpoint, slot_index, slot_index - NZ)
    squared = column_shell[:, None] + signed[None, :] * signed[None, :]
    inside = squared <= CUT2
    shells = squared.astype(jnp.float32)
    screen = screening[0]
    precond = MIXING * shells / (shells + screen)
    metric = jnp.where(inside, (shells + screen) / shells, jnp.float32(0.0))
    inside_mask = inside.astype(jnp.float32)
    weight_total = jnp.sum(metric)
    history_rho = [history_density[position] for position in range(HIST - 1)]
    history_res = [history_residual[position] for position in range(HIST - 1)]
    prev_residual = source - response[None] * density_before
    density = density_now
    previous = density_before
    slab_list = []
    norm_list = []
    for iteration in range(ITERS):
        residual = source - response[None] * density
        history_rho.append((density - previous).astype(jnp.bfloat16))
        history_res.append((residual - prev_residual).astype(jnp.bfloat16))
        if len(history_rho) > HIST:
            history_rho = history_rho[1:]
            history_res = history_res[1:]
        residual_half = rounded(residual)
        margin_rows = []
        projections = []
        for first_entry in history_res:
            weighted = rounded(metric[None] * first_entry.astype(jnp.float32))
            margin_rows.append(jnp.stack([jnp.sum(weighted * second_entry.astype(jnp.float32)) for second_entry in history_res]))
            projections.append(jnp.sum(weighted * residual_half))
        margin = jnp.stack(margin_rows)
        projection = jnp.stack(projections)
        square = jnp.sum(metric[None] * residual * residual)
        symmetric = 0.5 * (margin + margin.T)
        factor = jnp.linalg.cholesky(symmetric)
        coefficient = jax.scipy.linalg.cho_solve((factor, True), projection)
        norm_list.append(jnp.sqrt(square / weight_total))
        rho_mix = density
        res_mix = residual
        for position in range(HIST):
            rho_mix = rho_mix - coefficient[position] * history_rho[position].astype(jnp.float32)
            res_mix = res_mix - coefficient[position] * history_res[position].astype(jnp.float32)
        new_density = inside_mask[None] * (rho_mix + precond[None] * res_mix)
        spectrum = lax.complex(new_density[0], new_density[1])
        field = jnp.fft.ifft(spectrum, axis=-1) * math.sqrt(NZ)
        planes = jnp.stack([jnp.real(field).T, jnp.imag(field).T]).astype(jnp.float32)
        planes = planes.reshape(2, NZ, N_COL, N_GRP, COL_DEV).transpose(0, 1, 3, 2, 4).reshape(2, NZ, COLS)
        slab_list.append(planes)
        previous = density
        prev_residual = residual
        density = new_density
    return (jnp.stack(slab_list), density, jnp.stack(norm_list))
```

```python
import functools
import math

import jax
import jax.numpy as jnp
import numpy as np
from jax import lax
from jax.experimental import pallas as pl
from jax.experimental.pallas import tpu as pltpu
from jax.sharding import PartitionSpec as P

HIST = 8
ITERS = 2
MIXING = 0.7
NZ = 768
COLS = 256
N_COL = 32
N_GRP = 4
ZB = NZ // N_COL
HALF = COLS // 2
CUT2 = (NZ // 2 - 1) ** 2
CH = 32
N_CH = COLS // CH
SUB = 16
PEAK = 255.0 / 128.0
SCALE = 1.0 / (math.sqrt(NZ) * PEAK)
MESH = pl.DeviceIdType.MESH
F32 = jnp.float32
BF16 = jnp.bfloat16


def plane_table():
    k = np.arange(NZ)
    angle = (k[:, None] * k[None, :] % NZ) * (2.0 * math.pi / NZ)
    both = np.concatenate([np.cos(angle), np.sin(angle)], axis=1) * PEAK
    return jnp.asarray(both.astype(np.float32)).astype(BF16)


def nt_dot(left, right, precision=None):
    return lax.dot_general(
        left, right, (((1,), (1,)), ((), ())), precision=precision, preferred_element_type=F32
    )


def kernel(
    dn_h, db_h, src_h, resp_h, hd_h, hr_h, cs_s, scr_s, tab_h,
    slab_o, mix_o, norm_o,
    dn, db, src, resp, hd, hr, tab, d1, met, pre, w, w2, acc, acc2, sq, fold, amat, cvec,
    rmat, prod, pay, got,
    load_sem, late_sem, tab_sem, own_sem, send_sem, recv_sem, rsend_sem, rrecv_sem,
):
    col, grp = lax.axis_index("col"), lax.axis_index("grp")
    me = col * N_GRP + grp
    y0, z0, c0 = col // 8, (col // 2) % 4, col % 2

    def early(ch):
        rows = pl.ds(pl.multiple_of(ch * CH, CH), CH)
        return [
            pltpu.make_async_copy(dn_h.at[:, rows], dn.at[:, rows], load_sem.at[ch]),
            pltpu.make_async_copy(db_h.at[:, rows], db.at[:, rows], load_sem.at[ch]),
            pltpu.make_async_copy(src_h.at[:, rows], src.at[:, rows], load_sem.at[ch]),
            pltpu.make_async_copy(resp_h.at[rows], resp.at[rows], load_sem.at[ch]),
            pltpu.make_async_copy(hr_h.at[:, :, rows], hr.at[0:7, :, rows], load_sem.at[ch]),
        ]

    for ch in range(N_CH):
        for copy in early(ch):
            copy.start()
    late = pltpu.make_async_copy(hd_h, hd.at[0:7], late_sem)
    late.start()
    table = pltpu.make_async_copy(tab_h, tab, tab_sem)
    table.start()

    barrier = pltpu.get_barrier_semaphore()

    def peer(s):
        y = (y0 + 2 + s // 32) % 4
        z = (z0 + 2 + (s // 8) % 4) % 4
        x = (grp + 2 + (s // 2) % 4) % 4
        c = (c0 + s) % 2
        return y * 8 + z * 2 + c, x

    def others(body):
        def step(s, carry):
            body(*peer(s + (s >= 84).astype(jnp.int32)))
            return carry

        lax.fori_loop(0, 127, step, 0)

    others(
        lambda a, g: pl.semaphore_signal(barrier, inc=1, device_id=(a, g), device_id_type=MESH)
    )

    screen = scr_s[0]
    lane = lax.broadcasted_iota(jnp.int32, (8, NZ), 1)
    signed = jnp.where(lane < NZ // 2, lane, lane - NZ)
    signed2 = signed * signed
    row128 = lax.broadcasted_iota(jnp.int32, (8, 128), 0)
    lane128 = lax.broadcasted_iota(jnp.int32, (8, 128), 1)
    sq[...] = jnp.zeros_like(sq)
    acc[...] = jnp.zeros_like(acc)
    w2[...] = jnp.zeros_like(w2)
    acc2[...] = jnp.zeros_like(acc2)

    def geometry(i, total):
        base = pl.multiple_of(i * 8, 8)
        column = jnp.zeros((8, 128), jnp.int32)
        for r in range(8):
            column = jnp.where(row128 == r, cs_s[base + r], column)
        squared = jnp.concatenate([column] * (NZ // 128), axis=1) + signed2
        shells = squared.astype(F32)
        ratio = (shells + screen) / shells
        metric = jnp.where(squared <= CUT2, ratio, 0.0)
        met[pl.ds(base, 8)] = metric
        pre[pl.ds(base, 8)] = MIXING * shells / (shells + screen)
        return total + metric

    weight_rows = lax.fori_loop(0, COLS // 8, geometry, jnp.zeros((8, NZ), F32))

    def first(ch, carry):
        for copy in early(ch):
            copy.wait()
        for u in range(CH // SUB):
            rows = pl.ds(pl.multiple_of(ch * CH + u * SUB, SUB), SUB)
            metric = met[rows]
            r = resp[rows]
            for p in range(2):
                s = src[p, rows]
                residual = s - r * dn[p, rows]
                earlier = s - r * db[p, rows]
                hd[7, p, rows] = (dn[p, rows] - db[p, rows]).astype(BF16)
                hr[7, p, rows] = (residual - earlier).astype(BF16)
                hr[8, p, rows] = residual.astype(BF16)
                sq[...] += metric * residual * residual
                for i in range(HIST):
                    value = hr[i, p, rows].astype(F32)
                    w[p, i * CH + u * SUB : i * CH + (u + 1) * SUB] = (metric * value).astype(BF16)
        rows = pl.ds(pl.multiple_of(ch * CH, CH), CH)
        total = acc[...]
        for p in range(2):
            total = total + nt_dot(hr[:, p, rows].reshape(9 * CH, NZ), w[p])
        acc[...] = total
        return carry

    lax.fori_loop(0, N_CH, first, 0)

    def fold3(rows):
        return rows[:, :256] + rows[:, 256:512] + rows[:, 512:]

    def group_sums(lanes):
        l = lax.broadcasted_iota(jnp.int32, (lanes, 128), 0)
        j = lax.broadcasted_iota(jnp.int32, (lanes, 128), 1)
        return jnp.where(l // CH == j, 1.0, 0.0).astype(F32)

    def diagonal(total):
        r = lax.broadcasted_iota(jnp.int32, total.shape, 0)
        l = lax.broadcasted_iota(jnp.int32, total.shape, 1)
        kept = jnp.where(r % CH == l % CH, total, 0.0)
        return jnp.sum(kept.reshape(total.shape[0] // CH, CH, total.shape[1]), axis=1)

    def pack(slot, groups):
        ones = group_sums(groups)
        both = lax.dot_general(
            fold[:, :groups], ones, (((1,), (0,)), ((), ())),
            precision=lax.Precision.HIGHEST, preferred_element_type=F32,
        )
        upper = pltpu.roll(both[:8], 0, 1, stride=8, stride_axis=0)
        lower = pltpu.roll(both[8:], 64, 1, stride=8, stride_axis=0)
        row = jnp.sum(upper + lower, axis=0, keepdims=True)
        pay[slot] = row
        got[slot, pl.ds(me, 1)] = row.reshape(1, 1, 128)

    def spread(slot):
        def go(a, g):
            pltpu.make_async_remote_copy(
                src_ref=pay.at[slot],
                dst_ref=got.at[slot, me],
                send_sem=rsend_sem.at[slot],
                recv_sem=rrecv_sem.at[slot],
                device_id=(a, g),
                device_id_type=MESH,
            ).start()

        others(go)

    def gathered(slot):
        whole = got.at[slot, 0:127]
        pltpu.make_async_copy(whole, whole, rsend_sem.at[slot]).wait()
        pltpu.make_async_copy(whole, whole, rrecv_sem.at[slot]).wait()
        return jnp.sum(got[slot].reshape(128, 128), axis=0, keepdims=True)

    def unpack(row):
        same = jnp.broadcast_to(row, (8, 128))
        out = same
        for i in range(1, 8):
            out = jnp.where(row128 == i, pltpu.roll(same, 128 - 8 * i, 1), out)
        return out

    def lanes_sum(row, start):
        lanes = lax.broadcasted_iota(jnp.int32, (1, 128), 1)
        kept = jnp.where((lanes >= start) & (lanes < start + 8), row, 0.0)
        return jnp.sum(kept, axis=1, keepdims=True)

    def flip(matrix):
        out = jnp.zeros((8, 128), F32)
        for j in range(8):
            row = jnp.broadcast_to(matrix[j : j + 1], (8, 128))
            column = jnp.sum(jnp.where(row128 == lane128, row, 0.0), axis=1, keepdims=True)
            out = jnp.where(lane128 == j, column, out)
        return out

    def solve(matrix, right):
        m = jnp.where(lane128 < 8, matrix, jnp.where(lane128 == 8, right, 0.0))
        for k in range(8):
            row = m[k : k + 1] / m[k : k + 1, k : k + 1]
            m = jnp.where(row128 == k, row, m - m[:, k : k + 1] * row)
        return jnp.broadcast_to(m[:, 8:9], (8, NZ))

    fold[...] = jnp.zeros_like(fold)
    fold[0:9] = diagonal(acc[...])
    fold[9:10] = fold3(jnp.sum(sq[...], axis=0, keepdims=True))
    fold[10:11] = fold3(jnp.sum(weight_rows, axis=0, keepdims=True))
    pl.semaphore_wait(barrier, 127)
    pack(0, 256)
    spread(0)
    late.wait()
    table.wait()
    row = gathered(0)
    margin = unpack(row)
    margin = 0.5 * (margin + flip(margin))
    amat[...] = jnp.where(lane128 < 8, margin, 0.0)
    lanes8 = jnp.broadcast_to(pltpu.roll(row, 64, 1), (8, 128))
    right = jnp.sum(jnp.where(row128 == lane128, lanes8, 0.0), axis=1, keepdims=True)
    weight_total = lanes_sum(row, 80)
    norm0 = jnp.sqrt(lanes_sum(row, 72) / weight_total)
    cvec[...] = solve(amat[...], right)

    def mix(t, h, old, new):
        def step(i, carry):
            local = pl.multiple_of(i * SUB, SUB)
            rows = pl.ds(pl.multiple_of(h * HALF + i * SUB, SUB), SUB)
            r = resp[rows]
            inside = met[rows] > 0.0
            precond = pre[rows]
            values = []
            for p in range(2):
                density = old[p, rows]
                rho = density
                res = src[p, rows] - r * density
                for j in range(HIST):
                    c = cvec[j : j + 1]
                    rho = rho - c * hd[t + j, p, rows].astype(F32)
                    res = res - c * hr[t + j, p, rows].astype(F32)
                mixed = jnp.where(inside, rho + precond * res, 0.0)
                new[p, rows] = mixed
                values.append(mixed * SCALE)
            re, im = values[0].astype(BF16), values[1].astype(BF16)
            rmat[pl.ds(local, SUB), :NZ] = re
            rmat[pl.ds(local, SUB), NZ:] = (-values[1]).astype(BF16)
            rmat[pl.ds(HALF + local, SUB), :NZ] = im
            rmat[pl.ds(HALF + local, SUB), NZ:] = re
            return carry

        lax.fori_loop(0, HALF // SUB, step, 0)
        planes = nt_dot(tab[...], rmat[...])
        prod[t, h, 0] = planes[:, :HALF]
        prod[t, h, 1] = planes[:, HALF:]

    def out_block(t, h):
        return slab_o.at[t, :, :, pl.ds(pl.multiple_of(col * COLS + h * HALF, HALF), HALF)]

    def block(t, h, a):
        return prod.at[t, h, :, pl.ds(pl.multiple_of(a * ZB, 8), ZB)]

    def send(t, h):
        def step(s, carry):
            pair = s // 2
            z = (z0 + pair) % 4
            y = (y0 + pair // 4 + pair) % 4
            a = y * 8 + z * 2 + (c0 + s) % 2
            pltpu.make_async_remote_copy(
                src_ref=block(t, h, a),
                dst_ref=out_block(t, h),
                send_sem=send_sem.at[t],
                recv_sem=recv_sem.at[t],
                device_id=(a, grp),
                device_id_type=MESH,
            ).start()
            return carry

        lax.fori_loop(1, N_COL, step, 0)
        pltpu.make_async_copy(block(t, h, col), out_block(t, h), own_sem).start()

    def finish(t):
        for h in range(2):
            pltpu.make_async_copy(block(t, h, col), out_block(t, h), own_sem).wait()
        rows = (N_COL - 1) * COLS
        whole = slab_o.at[t, :, :, 0:rows]
        pltpu.make_async_copy(whole, whole, send_sem.at[t]).wait()
        pltpu.make_async_copy(whole, whole, recv_sem.at[t]).wait()

    mix(0, 0, dn, d1)
    send(0, 0)
    mix(0, 1, dn, d1)

    sq[...] = jnp.zeros_like(sq)

    def second(ch, carry):
        for u in range(CH // SUB):
            rows = pl.ds(pl.multiple_of(ch * CH + u * SUB, SUB), SUB)
            metric = met[rows]
            r = resp[rows]
            for p in range(2):
                s = src[p, rows]
                residual = s - r * d1[p, rows]
                earlier = s - r * dn[p, rows]
                hd[8, p, rows] = (d1[p, rows] - dn[p, rows]).astype(BF16)
                newest = (residual - earlier).astype(BF16)
                hr[8, p, rows] = newest
                sq[...] += metric * residual * residual
                half = residual.astype(BF16).astype(F32)
                w2[p, u * SUB : (u + 1) * SUB] = (metric * newest.astype(F32)).astype(BF16)
                w2[p, CH + u * SUB : CH + (u + 1) * SUB] = (metric * half).astype(BF16)
        rows = pl.ds(pl.multiple_of(ch * CH, CH), CH)
        total = acc2[...]
        for p in range(2):
            total = total + nt_dot(hr[1:9, p, rows].reshape(8 * CH, NZ), w2[p])
        acc2[...] = total
        return carry

    lax.fori_loop(0, N_CH, second, 0)
    fold[...] = jnp.zeros_like(fold)
    fold[0:8, 0:128] = diagonal(acc2[...])
    squares = fold3(jnp.sum(sq[...], axis=0, keepdims=True))
    fold[8:9, 0:128] = squares[:, :128] + squares[:, 128:]
    pack(1, 128)
    spread(1)
    send(0, 1)
    row = gathered(1)
    table1 = unpack(row)
    newest = table1[:, 0:1]
    across = jnp.sum(jnp.where(row128 == lane128, newest, 0.0), axis=0, keepdims=True)
    shifted = pltpu.roll(pltpu.roll(amat[...], 7, 0), 127, 1)
    matrix = jnp.where(lane128 == 7, newest, jnp.where(row128 == 7, across, shifted))
    norm1 = jnp.sqrt(lanes_sum(row, 64) / weight_total)
    cvec[...] = solve(matrix, table1[:, 1:2])

    mix(1, 0, d1, mix_o)
    send(1, 0)
    mix(1, 1, d1, mix_o)
    send(1, 1)
    lanes = lax.broadcasted_iota(jnp.int32, (1, 128), 1)
    norm_o[...] = jnp.where(lanes == 0, norm0, jnp.where(lanes == 1, norm1, 0.0))
    finish(0)
    finish(1)


def deliver(slab_v, mix_v, norm_v, slab_o, mix_o, norm_o, sem):
    copies = (
        pltpu.make_async_copy(slab_v, slab_o, sem.at[0]),
        pltpu.make_async_copy(mix_v, mix_o, sem.at[1]),
    )
    for copy in copies:
        copy.start()
    lanes = lax.broadcasted_iota(jnp.int32, (1, 128), 1)
    for t in range(ITERS):
        norm_o[t] = jnp.sum(jnp.where(lanes == t, norm_v[...], 0.0))
    for copy in copies:
        copy.wait()


def body(dn, db, src, resp, hd, hr, shell, screening):
    any_spec = pl.BlockSpec(memory_space=pl.ANY)
    hbm = pl.BlockSpec(memory_space=pltpu.HBM)
    smem = pl.BlockSpec(memory_space=pltpu.SMEM)
    stack = (2, COLS, NZ)
    vmem = pl.BlockSpec(memory_space=pltpu.VMEM)
    slab_shape = (ITERS, 2, ZB, N_COL * COLS)
    parts = pl.pallas_call(
        kernel,
        out_shape=(pltpu.VMEM(slab_shape, F32), pltpu.VMEM(stack, F32), pltpu.VMEM((1, 128), F32)),
        in_specs=[hbm] * 6 + [smem, smem, hbm],
        out_specs=(vmem, vmem, vmem),
        scratch_shapes=[
            pltpu.VMEM(stack, F32),
            pltpu.VMEM(stack, F32),
            pltpu.VMEM(stack, F32),
            pltpu.VMEM((COLS, NZ), F32),
            pltpu.VMEM((9,) + stack, BF16),
            pltpu.VMEM((9,) + stack, BF16),
            pltpu.VMEM((NZ, 2 * NZ), BF16),
            pltpu.VMEM(stack, F32),
            pltpu.VMEM((COLS, NZ), F32),
            pltpu.VMEM((COLS, NZ), F32),
            pltpu.VMEM((2, HIST * CH, NZ), BF16),
            pltpu.VMEM((2, 128, NZ), BF16),
            pltpu.VMEM((9 * CH, HIST * CH), F32),
            pltpu.VMEM((8 * CH, 128), F32),
            pltpu.VMEM((SUB, NZ), F32),
            pltpu.VMEM((16, 256), F32),
            pltpu.VMEM((8, 128), F32),
            pltpu.VMEM((8, NZ), F32),
            pltpu.VMEM((COLS, 2 * NZ), BF16),
            pltpu.VMEM((ITERS, 2, 2, NZ, HALF), F32),
            pltpu.VMEM((2, 1, 128), F32),
            pltpu.VMEM((2, N_COL * N_GRP, 1, 128), F32),
            pltpu.SemaphoreType.DMA((N_CH,)),
            pltpu.SemaphoreType.DMA,
            pltpu.SemaphoreType.DMA,
            pltpu.SemaphoreType.DMA,
            pltpu.SemaphoreType.DMA((ITERS,)),
            pltpu.SemaphoreType.DMA((ITERS,)),
            pltpu.SemaphoreType.DMA((2,)),
            pltpu.SemaphoreType.DMA((2,)),
        ],
        compiler_params=pltpu.CompilerParams(
            collective_id=0, has_side_effects=True, vmem_limit_bytes=54 * 1024 * 1024
        ),
        name="mixing",
    )(dn, db, src, resp, hd, hr, shell, screening, plane_table())
    return pl.pallas_call(
        deliver,
        out_shape=(
            jax.ShapeDtypeStruct(slab_shape, F32),
            jax.ShapeDtypeStruct(stack, F32),
            jax.ShapeDtypeStruct((ITERS,), F32),
        ),
        in_specs=[vmem, vmem, vmem],
        out_specs=(any_spec, any_spec, smem),
        scratch_shapes=[pltpu.SemaphoreType.DMA((2,))],
        compiler_params=pltpu.CompilerParams(vmem_limit_bytes=16 * 1024 * 1024),
        name="deliver",
    )(*parts)


def solution(mesh):
    columns = ("col", "grp")
    return jax.shard_map(
        body,
        mesh=mesh,
        in_specs=(
            P(None, columns, None),
            P(None, columns, None),
            P(None, columns, None),
            P(columns, None),
            P(None, None, columns, None),
            P(None, None, columns, None),
            P(columns),
            P(),
        ),
        out_specs=(P(None, None, "col", "grp"), P(None, columns, None), P()),
        check_vma=False,
    )
```

```python
import functools
import math

import jax
import jax.numpy as jnp
import numpy as np
from jax import lax
from jax.experimental import pallas as pl
from jax.experimental.pallas import tpu as pltpu
from jax.sharding import PartitionSpec as P

HIST = 8
ITERS = 2
MIXING = 0.7
NZ = 768
COLS = 256
N_COL = 32
N_GRP = 4
ZB = NZ // N_COL
HALF = COLS // 2
CUT2 = (NZ // 2 - 1) ** 2
CH = 32
N_CH = COLS // CH
SUB = 16
PEAK = 255.0 / 128.0
SCALE = 1.0 / (math.sqrt(NZ) * PEAK)
MESH = pl.DeviceIdType.MESH
F32 = jnp.float32
BF16 = jnp.bfloat16


def plane_table():
    k = np.arange(NZ)
    angle = (k[:, None] * k[None, :] % NZ) * (2.0 * math.pi / NZ)
    both = np.concatenate([np.cos(angle), np.sin(angle)], axis=1) * PEAK
    return jnp.asarray(both.astype(np.float32)).astype(BF16)


def nt_dot(left, right, precision=None):
    return lax.dot_general(
        left, right, (((1,), (1,)), ((), ())), precision=precision, preferred_element_type=F32
    )


def kernel(
    dn_h, db_h, src_h, resp_h, hd_h, hr_h, cs_h, scr_h, tab_h,
    slab_o, mix_o, norm_o,
    cs_m, scr_m, dn, db, src, resp, hd, hr, hn, tab, d1, met, pre, base, step, w0, w1, x0, x1, w2, acc, sq, weights,
    fold, amat, cvec, rmat, prod, whole, pay, gota,
    small_sem, load_sem, late_sem, tab_sem, own_sem, send_sem, recv_sem, rsend_sem, rrecv_sem,
):
    col, grp = lax.axis_index("col"), lax.axis_index("grp")
    ys = [(col // 8 + d) % 4 * 8 for d in range(4)]
    zs = [(col // 2 + d) % 4 * 2 for d in range(4)]
    cs = [col % 2, (col + 1) % 2]
    place = {1: 0, 3: 1, 2: 2, 0: 3}
    near = [(1, 2), (3, 2), (1, 1), (3, 3), (1, 3), (3, 1), (1, 0), (3, 0)]
    far = [(2, 2), (0, 2), (2, 1), (2, 3), (2, 0), (0, 1), (0, 3), (0, 0)]
    last = [
        (2, 2), (2, 1), (2, 3), (1, 2), (3, 2), (2, 0), (0, 2), (1, 1),
        (3, 3), (1, 3), (3, 1), (0, 0), (1, 0), (3, 0), (0, 1), (0, 3),
    ]
    others_all = [
        (ys[dy] + zs[dz] + cs[dc], (grp + dx) % 4)
        for dy in (2, 1, 3, 0) for dz in (2, 1, 3, 0) for dx in (2, 1, 3, 0) for dc in (1, 0)
        if dx or dy or dz or dc
    ]
    def early(ch):
        rows = pl.ds(pl.multiple_of(ch * CH, CH), CH)
        return [
            pltpu.make_async_copy(dn_h.at[:, rows], dn.at[:, rows], load_sem.at[ch]),
            pltpu.make_async_copy(db_h.at[:, rows], db.at[:, rows], load_sem.at[ch]),
            pltpu.make_async_copy(src_h.at[:, rows], src.at[:, rows], load_sem.at[ch]),
            pltpu.make_async_copy(resp_h.at[rows], resp.at[rows], load_sem.at[ch]),
            pltpu.make_async_copy(hr_h.at[:, :, rows], hr.at[:, :, rows], load_sem.at[ch]),
        ]

    small = [
        pltpu.make_async_copy(cs_h, cs_m, small_sem.at[0]),
        pltpu.make_async_copy(scr_h, scr_m, small_sem.at[1]),
    ]
    for copy in small:
        copy.start()
    for ch in range(N_CH):
        for copy in early(ch):
            copy.start()
    late = pltpu.make_async_copy(hd_h, hd, late_sem)
    table = [
        pltpu.make_async_copy(
            tab_h.at[pl.ds(pl.multiple_of(ys[dy] * ZB, 8 * ZB), 8 * ZB)],
            tab.at[place[dy] * 8 * ZB : (place[dy] + 1) * 8 * ZB],
            tab_sem.at[dy],
        )
        for dy in range(4)
    ]

    barrier = pltpu.get_barrier_semaphore()
    for peer in others_all:
        pl.semaphore_signal(barrier, inc=1, device_id=peer, device_id_type=MESH)

    for copy in small:
        copy.wait()
    screen = scr_m[0]
    lane = lax.broadcasted_iota(jnp.int32, (8, NZ), 1)
    signed = jnp.where(lane < NZ // 2, lane, lane - NZ)
    signed2 = signed * signed
    row128 = lax.broadcasted_iota(jnp.int32, (8, 128), 0)
    lane128 = lax.broadcasted_iota(jnp.int32, (8, 128), 1)
    sq[...] = jnp.zeros_like(sq)
    acc[...] = jnp.zeros_like(acc)
    weights[...] = jnp.zeros_like(weights)

    def geometry(first_row):
        column = jnp.zeros((8, 128), jnp.int32)
        for r in range(8):
            column = jnp.where(row128 == r, cs_m[first_row + r], column)
        squared = jnp.concatenate([column] * (NZ // 128), axis=1) + signed2
        shells = squared.astype(F32)
        metric = jnp.where(squared <= CUT2, (shells + screen) / shells, 0.0)
        met[pl.ds(first_row, 8)] = metric
        pre[pl.ds(first_row, 8)] = MIXING * shells / (shells + screen)
        weights[...] += metric

    def weigh(ch, w, x):
        for copy in early(ch):
            copy.wait()
        for u in range(CH // 8):
            geometry(pl.multiple_of(ch * CH + u * 8, 8))
        for u in range(CH // SUB):
            rows = pl.ds(pl.multiple_of(ch * CH + u * SUB, SUB), SUB)
            here = slice(u * SUB, (u + 1) * SUB)
            metric = met[rows]
            r = resp[rows]
            for p in range(2):
                s = src[p, rows]
                residual = s - r * dn[p, rows]
                earlier = s - r * db[p, rows]
                newest = (residual - earlier).astype(BF16)
                hn[0, p, rows] = newest
                x[p, here] = newest
                x[p, CH + u * SUB : CH + (u + 1) * SUB] = residual.astype(BF16)
                sq[...] += metric * residual * residual
                for i in range(HIST):
                    value = (hr[i, p, rows] if i < HIST - 1 else newest).astype(F32)
                    w[p, i * CH + u * SUB : i * CH + (u + 1) * SUB] = (metric * value).astype(BF16)

    def multiply(ch, w, x):
        rows = pl.ds(pl.multiple_of(ch * CH, CH), CH)
        for p in range(2):
            pairs = [hr[:, p, rows].reshape(7 * CH, NZ), x[p]]
            acc[p] = acc[p] + nt_dot(jnp.concatenate(pairs, axis=0), w[p])

    weigh(0, w0, x0)

    def first(i, carry):
        weigh(2 * i + 1, w1, x1)
        multiply(2 * i, w0, x0)
        weigh(2 * i + 2, w0, x0)
        multiply(2 * i + 1, w1, x1)
        return carry

    lax.fori_loop(0, N_CH // 2 - 1, first, 0)
    late.start()
    for copy in table:
        copy.start()
    weigh(N_CH - 1, w1, x1)
    multiply(N_CH - 2, w0, x0)
    multiply(N_CH - 1, w1, x1)

    def fold3(rows):
        return rows[:, :256] + rows[:, 256:512] + rows[:, 512:]

    def group_sums(lanes):
        l = lax.broadcasted_iota(jnp.int32, (lanes, 128), 0)
        j = lax.broadcasted_iota(jnp.int32, (lanes, 128), 1)
        return jnp.where(l // CH == j, 1.0, 0.0).astype(F32)

    def diagonal(total):
        r = lax.broadcasted_iota(jnp.int32, total.shape, 0)
        l = lax.broadcasted_iota(jnp.int32, total.shape, 1)
        kept = jnp.where(r % CH == l % CH, total, 0.0)
        return jnp.sum(kept.reshape(total.shape[0] // CH, CH, total.shape[1]), axis=1)

    def pack(groups):
        ones = group_sums(groups)
        both = lax.dot_general(
            fold[:, :groups], ones, (((1,), (0,)), ((), ())),
            precision=lax.Precision.HIGHEST, preferred_element_type=F32,
        )
        upper = pltpu.roll(both[:8], 0, 1, stride=8, stride_axis=0)
        lower = pltpu.roll(both[8:], 64, 1, stride=8, stride_axis=0)
        return jnp.sum(upper + lower, axis=0, keepdims=True)

    def spread(slot, row, got, place, peers):
        pay[slot] = row
        got[slot, pl.ds(place, 1)] = row.reshape(1, 1, 128)
        for peer in peers:
            pltpu.make_async_remote_copy(
                src_ref=pay.at[slot],
                dst_ref=got.at[slot, place],
                send_sem=rsend_sem.at[slot],
                recv_sem=rrecv_sem.at[slot],
                device_id=peer,
                device_id_type=MESH,
            ).start()

    def gathered(slot, got, peers):
        sent = got.at[slot, 0 : len(peers)]
        pltpu.make_async_copy(sent, sent, rsend_sem.at[slot]).wait()
        pltpu.make_async_copy(sent, sent, rrecv_sem.at[slot]).wait()
        rows = got[slot].reshape(len(peers) + 1, 128)
        return jnp.sum(rows, axis=0, keepdims=True)

    def unpack(row):
        same = jnp.broadcast_to(row, (8, 128))
        out = same
        for i in range(1, 8):
            out = jnp.where(row128 == i, pltpu.roll(same, 128 - 8 * i, 1), out)
        return out

    def lanes_sum(row, start):
        lanes = lax.broadcasted_iota(jnp.int32, (1, 128), 1)
        kept = jnp.where((lanes >= start) & (lanes < start + 8), row, 0.0)
        return jnp.sum(kept, axis=1, keepdims=True)

    def flip(matrix):
        out = jnp.zeros((8, 128), F32)
        for j in range(8):
            row = jnp.broadcast_to(matrix[j : j + 1], (8, 128))
            column = jnp.sum(jnp.where(row128 == lane128, row, 0.0), axis=1, keepdims=True)
            out = jnp.where(lane128 == j, column, out)
        return out

    def solve(matrix, right):
        m = jnp.where(lane128 < 8, matrix, jnp.where(lane128 == 8, right, 0.0))
        for k in range(8):
            column = jnp.broadcast_to(m[:, k : k + 1], (8, 128))
            row = m[k : k + 1] / column[k : k + 1]
            m = jnp.where(row128 == k, row, m - column * row)
        answer = jnp.broadcast_to(m[:, 8:9], (8, 128))
        for j in range(8):
            cvec[j] = jnp.broadcast_to(answer[j : j + 1], (8, 128))

    fold[...] = jnp.zeros_like(fold)
    fold[0:9] = diagonal(acc[0]) + diagonal(acc[1])
    fold[9:10] = fold3(jnp.sum(sq[...], axis=0, keepdims=True))
    fold[10:11] = fold3(jnp.sum(weights[...], axis=0, keepdims=True))
    row = pack(256)
    pl.semaphore_wait(barrier, len(others_all))
    spread(0, row, gota, col * N_GRP + grp, others_all)

    def prepare(i, carry):
        rows = pl.ds(pl.multiple_of(i * SUB, SUB), SUB)
        inside = met[rows] > 0.0
        precond = jnp.where(inside, pre[rows], 0.0)
        for p in range(2):
            density = dn[p, rows]
            residual = src[p, rows] - resp[rows] * density
            base[p, rows] = jnp.where(inside, density, 0.0) + precond * residual
            for j in range(HIST):
                if j < HIST - 1:
                    drho = hd[j, p, rows].astype(F32)
                else:
                    drho = (density - db[p, rows]).astype(BF16).astype(F32)
                dres = (hr[j, p, rows] if j < HIST - 1 else hn[0, p, rows]).astype(F32)
                step[j, p, rows] = jnp.where(inside, drho, 0.0) + precond * dres
        return carry

    late.wait()
    lax.fori_loop(0, COLS // SUB, prepare, 0)
    for copy in table:
        copy.wait()
    row = gathered(0, gota, others_all)
    margin = unpack(row)
    margin = 0.5 * (margin + flip(margin))
    amat[...] = jnp.where(lane128 < 8, margin, 0.0)
    lanes8 = jnp.broadcast_to(pltpu.roll(row, 64, 1), (8, 128))
    right = jnp.sum(jnp.where(row128 == lane128, lanes8, 0.0), axis=1, keepdims=True)
    weight_total = lanes_sum(row, 80)
    norm0 = jnp.sqrt(lanes_sum(row, 72) / weight_total)
    solve(amat[...], right)

    def mix(t, h, new):
        def go(i, carry):
            local = pl.multiple_of(i * SUB, SUB)
            rows = pl.ds(pl.multiple_of(h * HALF + i * SUB, SUB), SUB)
            coefficient = []
            for j in range(HIST):
                lanes = jnp.concatenate([cvec[j]] * (NZ // 128), axis=1)
                coefficient.append(jnp.concatenate([lanes] * (SUB // 8), axis=0))
            values = []
            for p in range(2):
                mixed = base[p, rows]
                for j in range(HIST):
                    mixed = mixed - coefficient[j] * step[t + j, p, rows]
                new[p, rows] = mixed
                values.append(mixed * SCALE)
            re, im = values[0].astype(BF16), values[1].astype(BF16)
            rmat[h, 0, pl.ds(local, SUB)] = re
            rmat[h, 0, pl.ds(HALF + local, SUB)] = im
            rmat[h, 1, pl.ds(local, SUB)] = im
            rmat[h, 1, pl.ds(HALF + local, SUB)] = (-values[0]).astype(BF16)
            return carry

        lax.fori_loop(0, HALF // SUB, go, 0)

    def transform(t, h, low, high):
        planes = nt_dot(tab[low:high, :NZ], rmat[h, 0]) - nt_dot(tab[low:high, NZ:], rmat[h, 1])
        for p in range(2):
            part = planes[:, p * HALF : (p + 1) * HALF]
            if t == 0:
                prod[h, p, low:high] = part
            else:
                whole[p, low:high, h * HALF : (h + 1) * HALF] = part

    def out_block(t, h):
        start, size = (col * COLS, COLS) if h is None else (col * COLS + h * HALF, HALF)
        return slab_o.at[t, :, :, pl.ds(pl.multiple_of(start, HALF), size)]

    def block(h, dy, dz, dc):
        start = place[dy] * 8 * ZB + (zs[dz] + cs[dc]) * ZB
        planes = whole if h is None else prod.at[h]
        return planes.at[:, pl.ds(pl.multiple_of(start, 8), ZB)]

    def own(t, h):
        return pltpu.make_async_copy(block(h, 0, 0, 0), out_block(t, h), own_sem)

    def send(t, h, pairs):
        for dy, dz in pairs:
            for dc in (1, 0):
                if dy or dz or dc:
                    pltpu.make_async_remote_copy(
                        src_ref=block(h, dy, dz, dc),
                        dst_ref=out_block(t, h),
                        send_sem=send_sem.at[t],
                        recv_sem=recv_sem.at[t],
                        device_id=(ys[dy] + zs[dz] + cs[dc], grp),
                        device_id_type=MESH,
                    ).start()
                else:
                    own(t, h).start()

    def finish(t):
        for h in (0, 1) if t == 0 else (None,):
            own(t, h).wait()
        rows = (N_COL - 1) * COLS
        blocks = slab_o.at[t, :, :, 0:rows]
        pltpu.make_async_copy(blocks, blocks, send_sem.at[t]).wait()
        pltpu.make_async_copy(blocks, blocks, recv_sem.at[t]).wait()

    mix(0, 0, d1)
    transform(0, 0, 0, NZ // 2)
    send(0, 0, near)
    transform(0, 0, NZ // 2, NZ)
    send(0, 0, far[:3])
    mix(0, 1, d1)

    sq[...] = jnp.zeros_like(sq)

    def second(i, carry):
        rows = pl.ds(pl.multiple_of(i * SUB, SUB), SUB)
        metric = met[rows]
        r = resp[rows]
        for p in range(2):
            s = src[p, rows]
            residual = s - r * d1[p, rows]
            earlier = s - r * dn[p, rows]
            newest = (residual - earlier).astype(BF16)
            hn[1, p, rows] = newest
            sq[...] += metric * residual * residual
            half = residual.astype(BF16).astype(F32)
            w2[p, 0, rows] = (metric * newest.astype(F32)).astype(BF16)
            w2[p, 1, rows] = (metric * half).astype(BF16)
        return carry

    def products():
        totals = [jnp.zeros((8 * CH, 2 * CH), F32)] * 2
        for ch in range(N_CH):
            rows = slice(ch * CH, (ch + 1) * CH)
            for p in range(2):
                pairs = [hr[1:7, p, rows].reshape(6 * CH, NZ), hn[0, p, rows], hn[1, p, rows]]
                totals[p] = totals[p] + nt_dot(
                    jnp.concatenate(pairs, axis=0), w2[p, :, rows].reshape(2 * CH, NZ)
                )
        return diagonal(totals[0]) + diagonal(totals[1])

    lax.fori_loop(0, COLS // SUB, second, 0)
    total = products()
    fold[...] = jnp.zeros_like(fold)
    fold[0:8, 0 : 2 * CH] = total
    squares = fold3(jnp.sum(sq[...], axis=0, keepdims=True))
    fold[8:9, 0:128] = squares[:, :128] + squares[:, 128:]
    row = pack(128)
    spread(1, row, gota, col * N_GRP + grp, others_all)
    send(0, 0, far[3:])

    def renew(i, carry):
        rows = pl.ds(pl.multiple_of(i * SUB, SUB), SUB)
        inside = met[rows] > 0.0
        precond = jnp.where(inside, pre[rows], 0.0)
        for p in range(2):
            density = d1[p, rows]
            residual = src[p, rows] - resp[rows] * density
            base[p, rows] = jnp.where(inside, density, 0.0) + precond * residual
            drho = (density - dn[p, rows]).astype(BF16).astype(F32)
            dres = hn[1, p, rows].astype(F32)
            step[HIST, p, rows] = jnp.where(inside, drho, 0.0) + precond * dres
        return carry

    lax.fori_loop(0, COLS // SUB, renew, 0)
    transform(0, 1, 0, NZ)
    send(0, 1, near + far)
    row = gathered(1, gota, others_all)
    table1 = unpack(row)
    newest = table1[:, 0:1]
    across = jnp.sum(jnp.where(row128 == lane128, newest, 0.0), axis=0, keepdims=True)
    shifted = pltpu.roll(pltpu.roll(amat[...], 7, 0), 127, 1)
    matrix = jnp.where(lane128 == 7, newest, jnp.where(row128 == 7, across, shifted))
    norm1 = jnp.sqrt(lanes_sum(row, 64) / weight_total)
    solve(matrix, table1[:, 1:2])

    for h in range(2):
        mix(1, h, mix_o)
        transform(1, h, 0, NZ)
    send(1, None, last)
    lanes = lax.broadcasted_iota(jnp.int32, (1, 128), 1)
    norm_o[...] = jnp.where(lanes == 0, norm0, jnp.where(lanes == 1, norm1, 0.0))
    finish(0)
    finish(1)


def deliver(slab_v, mix_v, norm_v, slab_o, mix_o, norm_o, sem):
    copies = []
    for p in range(2):
        for t in range(ITERS):
            for z in range(0, ZB, 8):
                at = (t, p, pl.ds(z, 8))
                copies.append((slab_v.at[at], slab_o.at[at]))
        for k in range(0, COLS, COLS // 4):
            at = (p, pl.ds(k, COLS // 4))
            copies.append((mix_v.at[at], mix_o.at[at]))
    copies = [pltpu.make_async_copy(a, b, sem.at[i]) for i, (a, b) in enumerate(copies)]
    for copy in copies:
        copy.start()
    lanes = lax.broadcasted_iota(jnp.int32, (1, 128), 1)
    for t in range(ITERS):
        norm_o[t] = jnp.sum(jnp.where(lanes == t, norm_v[...], 0.0))
    for copy in copies:
        copy.wait()


def body(dn, db, src, resp, hd, hr, shell, screening):
    any_spec = pl.BlockSpec(memory_space=pl.ANY)
    hbm = pl.BlockSpec(memory_space=pltpu.HBM)
    smem = pl.BlockSpec(memory_space=pltpu.SMEM)
    stack = (2, COLS, NZ)
    vmem = pl.BlockSpec(memory_space=pltpu.VMEM)
    slab_shape = (ITERS, 2, ZB, N_COL * COLS)
    parts = pl.pallas_call(
        kernel,
        out_shape=(pltpu.VMEM(slab_shape, F32), pltpu.VMEM(stack, F32), pltpu.VMEM((1, 128), F32)),
        in_specs=[hbm] * 9,
        out_specs=(vmem, vmem, vmem),
        scratch_shapes=[
            pltpu.SMEM((COLS,), jnp.int32),
            pltpu.SMEM((1,), F32),
            pltpu.VMEM(stack, F32),
            pltpu.VMEM(stack, F32),
            pltpu.VMEM(stack, F32),
            pltpu.VMEM((COLS, NZ), F32),
            pltpu.VMEM((7,) + stack, BF16),
            pltpu.VMEM((7,) + stack, BF16),
            pltpu.VMEM((2,) + stack, BF16),
            pltpu.VMEM((NZ, 2 * NZ), BF16),
            pltpu.VMEM(stack, F32),
            pltpu.VMEM((COLS, NZ), F32),
            pltpu.VMEM((COLS, NZ), F32),
            pltpu.VMEM(stack, F32),
            pltpu.VMEM((9,) + stack, F32),
            pltpu.VMEM((2, HIST * CH, NZ), BF16),
            pltpu.VMEM((2, HIST * CH, NZ), BF16),
            pltpu.VMEM((2, 2 * CH, NZ), BF16),
            pltpu.VMEM((2, 2 * CH, NZ), BF16),
            pltpu.VMEM((2, 2, COLS, NZ), BF16),
            pltpu.VMEM((2, 9 * CH, HIST * CH), F32),
            pltpu.VMEM((SUB, NZ), F32),
            pltpu.VMEM((8, NZ), F32),
            pltpu.VMEM((16, 256), F32),
            pltpu.VMEM((8, 128), F32),
            pltpu.VMEM((8, 8, 128), F32),
            pltpu.VMEM((2, 2, COLS, NZ), BF16),
            pltpu.VMEM((2, 2, NZ, HALF), F32),
            pltpu.VMEM((2, NZ, COLS), F32),
            pltpu.VMEM((2, 1, 128), F32),
            pltpu.VMEM((2, N_COL * N_GRP, 1, 128), F32),
            pltpu.SemaphoreType.DMA((2,)),
            pltpu.SemaphoreType.DMA((N_CH,)),
            pltpu.SemaphoreType.DMA,
            pltpu.SemaphoreType.DMA((4,)),
            pltpu.SemaphoreType.DMA,
            pltpu.SemaphoreType.DMA((ITERS,)),
            pltpu.SemaphoreType.DMA((ITERS,)),
            pltpu.SemaphoreType.DMA((2,)),
            pltpu.SemaphoreType.DMA((2,)),
        ],
        compiler_params=pltpu.CompilerParams(
            collective_id=0, has_side_effects=True, vmem_limit_bytes=54 * 1024 * 1024
        ),
        name="mixing",
    )(dn, db, src, resp, hd, hr, shell, screening, plane_table())
    return pl.pallas_call(
        deliver,
        out_shape=(
            jax.ShapeDtypeStruct(slab_shape, F32),
            jax.ShapeDtypeStruct(stack, F32),
            jax.ShapeDtypeStruct((ITERS,), F32),
        ),
        in_specs=[vmem, vmem, vmem],
        out_specs=(any_spec, any_spec, smem),
        scratch_shapes=[pltpu.SemaphoreType.DMA((20,))],
        compiler_params=pltpu.CompilerParams(vmem_limit_bytes=16 * 1024 * 1024),
        name="deliver",
    )(*parts)


def solution(mesh):
    columns = ("col", "grp")
    return jax.shard_map(
        body,
        mesh=mesh,
        in_specs=(
            P(None, columns, None),
            P(None, columns, None),
            P(None, columns, None),
            P(columns, None),
            P(None, None, columns, None),
            P(None, None, columns, None),
            P(columns),
            P(),
        ),
        out_specs=(P(None, None, "col", "grp"), P(None, columns, None), P()),
        check_vma=False,
    )
```

```python
import functools
import math

import jax
import jax.numpy as jnp
import numpy as np
from jax import lax
from jax.experimental import pallas as pl
from jax.experimental.pallas import tpu as pltpu
from jax.sharding import PartitionSpec as P

HIST = 8
ITERS = 2
MIXING = 0.7
NZ = 768
COLS = 256
N_COL = 32
N_GRP = 4
ZB = NZ // N_COL
HALF = COLS // 2
CUT2 = (NZ // 2 - 1) ** 2
CH = 32
N_CH = COLS // CH
SUB = 16
PEAK = 255.0 / 128.0
SCALE = 1.0 / (math.sqrt(NZ) * PEAK)
MESH = pl.DeviceIdType.MESH
F32 = jnp.float32
BF16 = jnp.bfloat16


def plane_table():
    k = np.arange(NZ)
    angle = (k[:, None] * k[None, :] % NZ) * (2.0 * math.pi / NZ)
    both = np.concatenate([np.cos(angle), np.sin(angle)], axis=1) * PEAK
    return jnp.asarray(both.astype(np.float32)).astype(BF16)


def nt_dot(left, right, precision=None):
    return lax.dot_general(
        left, right, (((1,), (1,)), ((), ())), precision=precision, preferred_element_type=F32
    )


def kernel(
    dn_h, db_h, src_h, resp_h, hd_h, hr_h, cs_h, scr_h, tab_h,
    slab_o, mix_o, norm_o,
    cs_m, scr_m, dn, db, src, resp, hd, hr, hn, tab, d1, met, pre, base, step, w0, w1, x0, x1, w2, acc, sq, weights,
    fold, amat, cvec, rmat, prod, whole, pay, gota,
    small_sem, load_sem, late_sem, tab_sem, own_sem, send_sem, recv_sem, rsend_sem, rrecv_sem,
):
    col, grp = lax.axis_index("col"), lax.axis_index("grp")
    ys = [(col // 8 + d) % 4 * 8 for d in range(4)]
    zs = [(col // 2 + d) % 4 * 2 for d in range(4)]
    cs = [col % 2, (col + 1) % 2]
    place = {1: 0, 3: 1, 2: 2, 0: 3}
    near = [(1, 2), (3, 2), (1, 1), (3, 3), (1, 3), (3, 1), (1, 0), (3, 0)]
    far = [(2, 2), (0, 2), (2, 1), (2, 3), (2, 0), (0, 1), (0, 3), (0, 0)]
    last = [
        (2, 2), (2, 1), (2, 3), (1, 2), (3, 2), (2, 0), (0, 2), (1, 1),
        (3, 3), (1, 3), (3, 1), (0, 0), (1, 0), (3, 0), (0, 1), (0, 3),
    ]
    others_all = [
        (ys[dy] + zs[dz] + cs[dc], (grp + dx) % 4)
        for dy in (2, 1, 3, 0) for dz in (2, 1, 3, 0) for dx in (2, 1, 3, 0) for dc in (1, 0)
        if dx or dy or dz or dc
    ]
    def early(ch):
        rows = pl.ds(pl.multiple_of(ch * CH, CH), CH)
        return [
            pltpu.make_async_copy(dn_h.at[:, rows], dn.at[:, rows], load_sem.at[ch]),
            pltpu.make_async_copy(db_h.at[:, rows], db.at[:, rows], load_sem.at[ch]),
            pltpu.make_async_copy(src_h.at[:, rows], src.at[:, rows], load_sem.at[ch]),
            pltpu.make_async_copy(resp_h.at[rows], resp.at[rows], load_sem.at[ch]),
            pltpu.make_async_copy(hr_h.at[:, :, rows], hr.at[:, :, rows], load_sem.at[ch]),
        ]

    small = [
        pltpu.make_async_copy(cs_h, cs_m, small_sem.at[0]),
        pltpu.make_async_copy(scr_h, scr_m, small_sem.at[1]),
    ]
    for copy in small:
        copy.start()
    for ch in range(N_CH):
        for copy in early(ch):
            copy.start()
    late = pltpu.make_async_copy(hd_h, hd, late_sem)
    table = [
        pltpu.make_async_copy(
            tab_h.at[pl.ds(pl.multiple_of(ys[dy] * ZB, 8 * ZB), 8 * ZB)],
            tab.at[place[dy] * 8 * ZB : (place[dy] + 1) * 8 * ZB],
            tab_sem.at[dy],
        )
        for dy in range(4)
    ]

    barrier = pltpu.get_barrier_semaphore()
    for peer in others_all:
        pl.semaphore_signal(barrier, inc=1, device_id=peer, device_id_type=MESH)

    for copy in small:
        copy.wait()
    screen = scr_m[0]
    lane = lax.broadcasted_iota(jnp.int32, (8, NZ), 1)
    signed = jnp.where(lane < NZ // 2, lane, lane - NZ)
    signed2 = signed * signed
    row128 = lax.broadcasted_iota(jnp.int32, (8, 128), 0)
    lane128 = lax.broadcasted_iota(jnp.int32, (8, 128), 1)
    sq[...] = jnp.zeros_like(sq)
    acc[...] = jnp.zeros_like(acc)
    weights[...] = jnp.zeros_like(weights)

    def geometry(first_row):
        column = jnp.zeros((8, 128), jnp.int32)
        for r in range(8):
            column = jnp.where(row128 == r, cs_m[first_row + r], column)
        squared = jnp.concatenate([column] * (NZ // 128), axis=1) + signed2
        shells = squared.astype(F32)
        metric = jnp.where(squared <= CUT2, (shells + screen) / shells, 0.0)
        met[pl.ds(first_row, 8)] = metric
        pre[pl.ds(first_row, 8)] = MIXING * shells / (shells + screen)
        weights[...] += metric

    def weigh(ch, w, x):
        for copy in early(ch):
            copy.wait()
        for u in range(CH // 8):
            geometry(pl.multiple_of(ch * CH + u * 8, 8))
        for u in range(CH // SUB):
            rows = pl.ds(pl.multiple_of(ch * CH + u * SUB, SUB), SUB)
            here = slice(u * SUB, (u + 1) * SUB)
            metric = met[rows]
            r = resp[rows]
            for p in range(2):
                s = src[p, rows]
                residual = s - r * dn[p, rows]
                earlier = s - r * db[p, rows]
                newest = (residual - earlier).astype(BF16)
                hn[0, p, rows] = newest
                x[p, here] = newest
                x[p, CH + u * SUB : CH + (u + 1) * SUB] = residual.astype(BF16)
                sq[...] += metric * residual * residual
                for i in range(HIST):
                    value = (hr[i, p, rows] if i < HIST - 1 else newest).astype(F32)
                    w[p, i * CH + u * SUB : i * CH + (u + 1) * SUB] = (metric * value).astype(BF16)

    def multiply(ch, w, x):
        rows = pl.ds(pl.multiple_of(ch * CH, CH), CH)
        for p in range(2):
            pairs = [hr[:, p, rows].reshape(7 * CH, NZ), x[p]]
            acc[p] = acc[p] + nt_dot(jnp.concatenate(pairs, axis=0), w[p])

    weigh(0, w0, x0)

    def first(i, carry):
        weigh(2 * i + 1, w1, x1)
        multiply(2 * i, w0, x0)
        weigh(2 * i + 2, w0, x0)
        multiply(2 * i + 1, w1, x1)
        return carry

    lax.fori_loop(0, N_CH // 2 - 1, first, 0)
    late.start()
    for copy in table:
        copy.start()
    weigh(N_CH - 1, w1, x1)
    multiply(N_CH - 2, w0, x0)
    multiply(N_CH - 1, w1, x1)

    def fold3(rows):
        return rows[:, :256] + rows[:, 256:512] + rows[:, 512:]

    def group_sums(lanes):
        l = lax.broadcasted_iota(jnp.int32, (lanes, 128), 0)
        j = lax.broadcasted_iota(jnp.int32, (lanes, 128), 1)
        return jnp.where(l // CH == j, 1.0, 0.0).astype(F32)

    def diagonal(total):
        r = lax.broadcasted_iota(jnp.int32, total.shape, 0)
        l = lax.broadcasted_iota(jnp.int32, total.shape, 1)
        kept = jnp.where(r % CH == l % CH, total, 0.0)
        return jnp.sum(kept.reshape(total.shape[0] // CH, CH, total.shape[1]), axis=1)

    def pack(groups):
        ones = group_sums(groups)
        both = lax.dot_general(
            fold[:, :groups], ones, (((1,), (0,)), ((), ())),
            precision=lax.Precision.HIGHEST, preferred_element_type=F32,
        )
        upper = pltpu.roll(both[:8], 0, 1, stride=8, stride_axis=0)
        lower = pltpu.roll(both[8:], 64, 1, stride=8, stride_axis=0)
        return jnp.sum(upper + lower, axis=0, keepdims=True)

    def spread(slot, row, got, place, peers):
        pay[slot] = row
        got[slot, pl.ds(place, 1)] = row.reshape(1, 1, 128)
        for peer in peers:
            pltpu.make_async_remote_copy(
                src_ref=pay.at[slot],
                dst_ref=got.at[slot, place],
                send_sem=rsend_sem.at[slot],
                recv_sem=rrecv_sem.at[slot],
                device_id=peer,
                device_id_type=MESH,
            ).start()

    def gathered(slot, got, peers):
        sent = got.at[slot, 0 : len(peers)]
        pltpu.make_async_copy(sent, sent, rsend_sem.at[slot]).wait()
        pltpu.make_async_copy(sent, sent, rrecv_sem.at[slot]).wait()
        rows = got[slot].reshape(len(peers) + 1, 128)
        return jnp.sum(rows, axis=0, keepdims=True)

    def unpack(row):
        same = jnp.broadcast_to(row, (8, 128))
        out = same
        for i in range(1, 8):
            out = jnp.where(row128 == i, pltpu.roll(same, 128 - 8 * i, 1), out)
        return out

    def lanes_sum(row, start):
        lanes = lax.broadcasted_iota(jnp.int32, (1, 128), 1)
        kept = jnp.where((lanes >= start) & (lanes < start + 8), row, 0.0)
        return jnp.sum(kept, axis=1, keepdims=True)

    def flip(matrix):
        out = jnp.zeros((8, 128), F32)
        for j in range(8):
            row = jnp.broadcast_to(matrix[j : j + 1], (8, 128))
            column = jnp.sum(jnp.where(row128 == lane128, row, 0.0), axis=1, keepdims=True)
            out = jnp.where(lane128 == j, column, out)
        return out

    def solve(matrix, right):
        m = jnp.where(lane128 < 8, matrix, jnp.where(lane128 == 8, right, 0.0))
        for k in range(8):
            column = jnp.broadcast_to(m[:, k : k + 1], (8, 128))
            row = m[k : k + 1] / column[k : k + 1]
            m = jnp.where(row128 == k, row, m - column * row)
        answer = jnp.broadcast_to(m[:, 8:9], (8, 128))
        for j in range(8):
            cvec[j] = jnp.broadcast_to(answer[j : j + 1], (8, 128))

    fold[...] = jnp.zeros_like(fold)
    fold[0:9] = diagonal(acc[0]) + diagonal(acc[1])
    fold[9:10] = fold3(jnp.sum(sq[...], axis=0, keepdims=True))
    fold[10:11] = fold3(jnp.sum(weights[...], axis=0, keepdims=True))
    row = pack(256)
    pl.semaphore_wait(barrier, len(others_all))
    spread(0, row, gota, col * N_GRP + grp, others_all)

    def prepare(i, carry):
        rows = pl.ds(pl.multiple_of(i * SUB, SUB), SUB)
        inside = met[rows] > 0.0
        precond = jnp.where(inside, pre[rows], 0.0)
        for p in range(2):
            density = dn[p, rows]
            residual = src[p, rows] - resp[rows] * density
            base[p, rows] = jnp.where(inside, density, 0.0) + precond * residual
            for j in range(HIST):
                if j < HIST - 1:
                    drho = hd[j, p, rows].astype(F32)
                else:
                    drho = (density - db[p, rows]).astype(BF16).astype(F32)
                dres = (hr[j, p, rows] if j < HIST - 1 else hn[0, p, rows]).astype(F32)
                step[j, p, rows] = jnp.where(inside, drho, 0.0) + precond * dres
        return carry

    late.wait()
    lax.fori_loop(0, COLS // SUB, prepare, 0)
    for copy in table:
        copy.wait()
    row = gathered(0, gota, others_all)
    margin = unpack(row)
    margin = 0.5 * (margin + flip(margin))
    amat[...] = jnp.where(lane128 < 8, margin, 0.0)
    lanes8 = jnp.broadcast_to(pltpu.roll(row, 64, 1), (8, 128))
    right = jnp.sum(jnp.where(row128 == lane128, lanes8, 0.0), axis=1, keepdims=True)
    weight_total = lanes_sum(row, 80)
    norm0 = jnp.sqrt(lanes_sum(row, 72) / weight_total)
    solve(amat[...], right)

    def mix(t, h, new):
        def go(i, carry):
            local = pl.multiple_of(i * SUB, SUB)
            rows = pl.ds(pl.multiple_of(h * HALF + i * SUB, SUB), SUB)
            coefficient = []
            for j in range(HIST):
                lanes = jnp.concatenate([cvec[j]] * (NZ // 128), axis=1)
                coefficient.append(jnp.concatenate([lanes] * (SUB // 8), axis=0))
            values = []
            for p in range(2):
                mixed = base[p, rows]
                for j in range(HIST):
                    mixed = mixed - coefficient[j] * step[t + j, p, rows]
                new[p, rows] = mixed
                values.append(mixed * SCALE)
            re, im = values[0].astype(BF16), values[1].astype(BF16)
            rmat[h, 0, pl.ds(local, SUB)] = re
            rmat[h, 0, pl.ds(HALF + local, SUB)] = im
            rmat[h, 1, pl.ds(local, SUB)] = im
            rmat[h, 1, pl.ds(HALF + local, SUB)] = (-values[0]).astype(BF16)
            return carry

        lax.fori_loop(0, HALF // SUB, go, 0)

    def transform(t, h, low, high):
        planes = nt_dot(tab[low:high, :NZ], rmat[h, 0]) - nt_dot(tab[low:high, NZ:], rmat[h, 1])
        for p in range(2):
            part = planes[:, p * HALF : (p + 1) * HALF]
            if t == 0:
                prod[h, p, low:high] = part
            else:
                whole[p, low:high, h * HALF : (h + 1) * HALF] = part

    def out_block(t, h):
        start, size = (col * COLS, COLS) if h is None else (col * COLS + h * HALF, HALF)
        return slab_o.at[t, :, :, pl.ds(pl.multiple_of(start, HALF), size)]

    def block(h, dy, dz, dc):
        start = place[dy] * 8 * ZB + (zs[dz] + cs[dc]) * ZB
        planes = whole if h is None else prod.at[h]
        return planes.at[:, pl.ds(pl.multiple_of(start, 8), ZB)]

    def own(t, h):
        return pltpu.make_async_copy(block(h, 0, 0, 0), out_block(t, h), own_sem)

    def send(t, h, pairs):
        for dy, dz in pairs:
            for dc in (1, 0):
                if dy or dz or dc:
                    pltpu.make_async_remote_copy(
                        src_ref=block(h, dy, dz, dc),
                        dst_ref=out_block(t, h),
                        send_sem=send_sem.at[t],
                        recv_sem=recv_sem.at[t],
                        device_id=(ys[dy] + zs[dz] + cs[dc], grp),
                        device_id_type=MESH,
                    ).start()
                else:
                    own(t, h).start()

    def finish(t):
        for h in (0, 1) if t == 0 else (None,):
            own(t, h).wait()
        rows = (N_COL - 1) * COLS
        blocks = slab_o.at[t, :, :, 0:rows]
        pltpu.make_async_copy(blocks, blocks, send_sem.at[t]).wait()
        pltpu.make_async_copy(blocks, blocks, recv_sem.at[t]).wait()

    mix(0, 0, d1)
    transform(0, 0, 0, NZ // 2)
    send(0, 0, near)
    transform(0, 0, NZ // 2, NZ)
    send(0, 0, far[:3])
    mix(0, 1, d1)

    sq[...] = jnp.zeros_like(sq)

    def second(i, carry):
        rows = pl.ds(pl.multiple_of(i * SUB, SUB), SUB)
        metric = met[rows]
        r = resp[rows]
        for p in range(2):
            s = src[p, rows]
            residual = s - r * d1[p, rows]
            earlier = s - r * dn[p, rows]
            newest = (residual - earlier).astype(BF16)
            hn[1, p, rows] = newest
            sq[...] += metric * residual * residual
            half = residual.astype(BF16).astype(F32)
            w2[p, 0, rows] = (metric * newest.astype(F32)).astype(BF16)
            w2[p, 1, rows] = (metric * half).astype(BF16)
        return carry

    def products():
        totals = [jnp.zeros((8 * CH, 2 * CH), F32)] * 2
        for ch in range(N_CH):
            rows = slice(ch * CH, (ch + 1) * CH)
            for p in range(2):
                pairs = [hr[1:7, p, rows].reshape(6 * CH, NZ), hn[0, p, rows], hn[1, p, rows]]
                totals[p] = totals[p] + nt_dot(
                    jnp.concatenate(pairs, axis=0), w2[p, :, rows].reshape(2 * CH, NZ)
                )
        return diagonal(totals[0]) + diagonal(totals[1])

    lax.fori_loop(0, COLS // SUB, second, 0)
    total = products()
    fold[...] = jnp.zeros_like(fold)
    fold[0:8, 0 : 2 * CH] = total
    squares = fold3(jnp.sum(sq[...], axis=0, keepdims=True))
    fold[8:9, 0:128] = squares[:, :128] + squares[:, 128:]
    row = pack(128)
    spread(1, row, gota, col * N_GRP + grp, others_all)
    send(0, 0, far[3:])

    def renew(i, carry):
        rows = pl.ds(pl.multiple_of(i * SUB, SUB), SUB)
        inside = met[rows] > 0.0
        precond = jnp.where(inside, pre[rows], 0.0)
        for p in range(2):
            density = d1[p, rows]
            residual = src[p, rows] - resp[rows] * density
            base[p, rows] = jnp.where(inside, density, 0.0) + precond * residual
            drho = (density - dn[p, rows]).astype(BF16).astype(F32)
            dres = hn[1, p, rows].astype(F32)
            step[HIST, p, rows] = jnp.where(inside, drho, 0.0) + precond * dres
        return carry

    lax.fori_loop(0, COLS // SUB, renew, 0)
    transform(0, 1, 0, NZ)
    send(0, 1, near + far)
    row = gathered(1, gota, others_all)
    table1 = unpack(row)
    newest = table1[:, 0:1]
    across = jnp.sum(jnp.where(row128 == lane128, newest, 0.0), axis=0, keepdims=True)
    shifted = pltpu.roll(pltpu.roll(amat[...], 7, 0), 127, 1)
    matrix = jnp.where(lane128 == 7, newest, jnp.where(row128 == 7, across, shifted))
    norm1 = jnp.sqrt(lanes_sum(row, 64) / weight_total)
    solve(matrix, table1[:, 1:2])

    for h in range(2):
        mix(1, h, mix_o)
        transform(1, h, 0, NZ)
    send(1, None, last)
    lanes = lax.broadcasted_iota(jnp.int32, (1, 128), 1)
    norm_o[...] = jnp.where(lanes == 0, norm0, jnp.where(lanes == 1, norm1, 0.0))
    finish(0)
    finish(1)


def deliver(slab_v, mix_v, norm_v, slab_o, mix_o, norm_o, norm_s, sem):
    copies = []
    for p in range(2):
        for t in range(ITERS):
            for z in range(0, ZB, 8):
                at = (t, p, pl.ds(z, 8))
                copies.append((slab_v.at[at], slab_o.at[at]))
        for k in range(0, COLS, COLS // 4):
            at = (p, pl.ds(k, COLS // 4))
            copies.append((mix_v.at[at], mix_o.at[at]))
    copies = [pltpu.make_async_copy(a, b, sem.at[i]) for i, (a, b) in enumerate(copies)]
    for copy in copies:
        copy.start()
    lanes = lax.broadcasted_iota(jnp.int32, (1, 128), 1)
    for t in range(ITERS):
        norm_s[t] = jnp.sum(jnp.where(lanes == t, norm_v[...], 0.0))
    norms = pltpu.make_async_copy(norm_s, norm_o, sem.at[len(copies)])
    norms.start()
    for copy in copies:
        copy.wait()
    norms.wait()


def body(dn, db, src, resp, hd, hr, shell, screening):
    hbm = pl.BlockSpec(memory_space=pltpu.HBM)
    stack = (2, COLS, NZ)
    vmem = pl.BlockSpec(memory_space=pltpu.VMEM)
    slab_shape = (ITERS, 2, ZB, N_COL * COLS)
    parts = pl.pallas_call(
        kernel,
        out_shape=(pltpu.VMEM(slab_shape, F32), pltpu.VMEM(stack, F32), pltpu.VMEM((1, 128), F32)),
        in_specs=[hbm] * 9,
        out_specs=(vmem, vmem, vmem),
        scratch_shapes=[
            pltpu.SMEM((COLS,), jnp.int32),
            pltpu.SMEM((1,), F32),
            pltpu.VMEM(stack, F32),
            pltpu.VMEM(stack, F32),
            pltpu.VMEM(stack, F32),
            pltpu.VMEM((COLS, NZ), F32),
            pltpu.VMEM((7,) + stack, BF16),
            pltpu.VMEM((7,) + stack, BF16),
            pltpu.VMEM((2,) + stack, BF16),
            pltpu.VMEM((NZ, 2 * NZ), BF16),
            pltpu.VMEM(stack, F32),
            pltpu.VMEM((COLS, NZ), F32),
            pltpu.VMEM((COLS, NZ), F32),
            pltpu.VMEM(stack, F32),
            pltpu.VMEM((9,) + stack, F32),
            pltpu.VMEM((2, HIST * CH, NZ), BF16),
            pltpu.VMEM((2, HIST * CH, NZ), BF16),
            pltpu.VMEM((2, 2 * CH, NZ), BF16),
            pltpu.VMEM((2, 2 * CH, NZ), BF16),
            pltpu.VMEM((2, 2, COLS, NZ), BF16),
            pltpu.VMEM((2, 9 * CH, HIST * CH), F32),
            pltpu.VMEM((SUB, NZ), F32),
            pltpu.VMEM((8, NZ), F32),
            pltpu.VMEM((16, 256), F32),
            pltpu.VMEM((8, 128), F32),
            pltpu.VMEM((8, 8, 128), F32),
            pltpu.VMEM((2, 2, COLS, NZ), BF16),
            pltpu.VMEM((2, 2, NZ, HALF), F32),
            pltpu.VMEM((2, NZ, COLS), F32),
            pltpu.VMEM((2, 1, 128), F32),
            pltpu.VMEM((2, N_COL * N_GRP, 1, 128), F32),
            pltpu.SemaphoreType.DMA((2,)),
            pltpu.SemaphoreType.DMA((N_CH,)),
            pltpu.SemaphoreType.DMA,
            pltpu.SemaphoreType.DMA((4,)),
            pltpu.SemaphoreType.DMA,
            pltpu.SemaphoreType.DMA((ITERS,)),
            pltpu.SemaphoreType.DMA((ITERS,)),
            pltpu.SemaphoreType.DMA((2,)),
            pltpu.SemaphoreType.DMA((2,)),
        ],
        compiler_params=pltpu.CompilerParams(
            collective_id=0, has_side_effects=True, vmem_limit_bytes=54 * 1024 * 1024
        ),
        name="mixing",
    )(dn, db, src, resp, hd, hr, shell, screening, plane_table())
    return pl.pallas_call(
        deliver,
        out_shape=(
            jax.ShapeDtypeStruct(slab_shape, F32),
            jax.ShapeDtypeStruct(stack, F32),
            jax.ShapeDtypeStruct((ITERS,), F32),
        ),
        in_specs=[vmem, vmem, vmem],
        out_specs=(hbm, hbm, hbm),
        scratch_shapes=[pltpu.SMEM((ITERS,), F32), pltpu.SemaphoreType.DMA((21,))],
        compiler_params=pltpu.CompilerParams(vmem_limit_bytes=16 * 1024 * 1024),
        name="deliver",
    )(*parts)


def solution(mesh):
    columns = ("col", "grp")
    return jax.shard_map(
        body,
        mesh=mesh,
        in_specs=(
            P(None, columns, None),
            P(None, columns, None),
            P(None, columns, None),
            P(columns, None),
            P(None, None, columns, None),
            P(None, None, columns, None),
            P(columns),
            P(),
        ),
        out_specs=(P(None, None, "col", "grp"), P(None, columns, None), P()),
        check_vma=False,
    )
```

```python
import functools
import math

import jax
import jax.numpy as jnp
import numpy as np
from jax import lax
from jax.experimental import pallas as pl
from jax.experimental.pallas import tpu as pltpu
from jax.sharding import PartitionSpec as P

HIST = 8
ITERS = 2
MIXING = 0.7
NZ = 768
COLS = 256
N_COL = 32
N_GRP = 4
ZB = NZ // N_COL
HALF = COLS // 2
CUT2 = (NZ // 2 - 1) ** 2
CH = 32
N_CH = COLS // CH
SUB = 16
PEAK = 255.0 / 128.0
SCALE = 1.0 / (math.sqrt(NZ) * PEAK)
MESH = pl.DeviceIdType.MESH
F32 = jnp.float32
BF16 = jnp.bfloat16


def plane_table():
    k = np.arange(NZ)
    angle = (k[:, None] * k[None, :] % NZ) * (2.0 * math.pi / NZ)
    both = np.concatenate([np.cos(angle), np.sin(angle)], axis=1) * PEAK
    return jnp.asarray(both.astype(np.float32)).astype(BF16)


def nt_dot(left, right, precision=None):
    return lax.dot_general(
        left, right, (((1,), (1,)), ((), ())), precision=precision, preferred_element_type=F32
    )


def kernel(
    dn_h, db_h, src_h, resp_h, hd_h, hr_h, cs_h, scr_h, tab_h,
    slab_o, mix_o, norm_o,
    cs_m, scr_m, dn, db, src, resp, hd, hr, hn, tab, d1, met, pre, base, step, w0, w1, x0, x1, w2, acc, sq, weights,
    fold, amat, cvec, rmat, prod, whole, pay, gota,
    small_sem, load_sem, late_sem, tab_sem, own_sem, send_sem, recv_sem, rsend_sem, rrecv_sem,
):
    col, grp = lax.axis_index("col"), lax.axis_index("grp")
    ys = [(col // 8 + d) % 4 * 8 for d in range(4)]
    zs = [(col // 2 + d) % 4 * 2 for d in range(4)]
    cs = [col % 2, (col + 1) % 2]
    place = {1: 0, 3: 1, 2: 2, 0: 3}
    near = [(1, 2), (3, 2), (1, 1), (3, 3), (1, 3), (3, 1), (1, 0), (3, 0)]
    far = [(2, 2), (0, 2), (2, 1), (2, 3), (2, 0), (0, 1), (0, 3), (0, 0)]
    last = [
        (2, 2), (2, 1), (2, 3), (1, 2), (3, 2), (2, 0), (0, 2), (1, 1),
        (3, 3), (1, 3), (3, 1), (0, 0), (1, 0), (3, 0), (0, 1), (0, 3),
    ]
    offsets = [
        (dy, dz, dx, dc)
        for dy in (2, 1, 3, 0) for dz in (2, 1, 3, 0) for dx in (2, 1, 3, 0) for dc in (1, 0)
        if dx or dy or dz or dc
    ]
    offsets.sort(key=lambda d: -sum(min(step, 4 - step) for step in d[:3]))
    others_all = [
        (ys[dy] + zs[dz] + cs[dc], (grp + dx) % 4) for dy, dz, dx, dc in offsets
    ]

    def early(ch):
        rows = pl.ds(pl.multiple_of(ch * CH, CH), CH)
        return [
            pltpu.make_async_copy(dn_h.at[:, rows], dn.at[:, rows], load_sem.at[ch]),
            pltpu.make_async_copy(db_h.at[:, rows], db.at[:, rows], load_sem.at[ch]),
            pltpu.make_async_copy(src_h.at[:, rows], src.at[:, rows], load_sem.at[ch]),
            pltpu.make_async_copy(resp_h.at[rows], resp.at[rows], load_sem.at[ch]),
            pltpu.make_async_copy(hr_h.at[:, :, rows], hr.at[:, :, rows], load_sem.at[ch]),
        ]

    small = [
        pltpu.make_async_copy(cs_h, cs_m, small_sem.at[0]),
        pltpu.make_async_copy(scr_h, scr_m, small_sem.at[1]),
    ]
    for copy in small:
        copy.start()
    for ch in range(N_CH):
        for copy in early(ch):
            copy.start()
    late = pltpu.make_async_copy(hd_h, hd, late_sem)
    table = [
        pltpu.make_async_copy(
            tab_h.at[pl.ds(pl.multiple_of(ys[dy] * ZB, 8 * ZB), 8 * ZB)],
            tab.at[place[dy] * 8 * ZB : (place[dy] + 1) * 8 * ZB],
            tab_sem.at[dy],
        )
        for dy in range(4)
    ]

    barrier = pltpu.get_barrier_semaphore()
    for peer in others_all:
        pl.semaphore_signal(barrier, inc=1, device_id=peer, device_id_type=MESH)

    for copy in small:
        copy.wait()
    screen = scr_m[0]
    lane = lax.broadcasted_iota(jnp.int32, (8, NZ), 1)
    signed = jnp.where(lane < NZ // 2, lane, lane - NZ)
    signed2 = signed * signed
    row128 = lax.broadcasted_iota(jnp.int32, (8, 128), 0)
    lane128 = lax.broadcasted_iota(jnp.int32, (8, 128), 1)
    sq[...] = jnp.zeros_like(sq)
    acc[...] = jnp.zeros_like(acc)
    weights[...] = jnp.zeros_like(weights)

    def geometry(first_row):
        column = jnp.zeros((8, 128), jnp.int32)
        for r in range(8):
            column = jnp.where(row128 == r, cs_m[first_row + r], column)
        squared = jnp.concatenate([column] * (NZ // 128), axis=1) + signed2
        shells = squared.astype(F32)
        metric = jnp.where(squared <= CUT2, (shells + screen) / shells, 0.0)
        met[pl.ds(first_row, 8)] = metric
        pre[pl.ds(first_row, 8)] = MIXING * shells / (shells + screen)
        weights[...] += metric

    def weigh(ch, w, x):
        for copy in early(ch):
            copy.wait()
        for u in range(CH // 8):
            geometry(pl.multiple_of(ch * CH + u * 8, 8))
        for u in range(CH // SUB):
            rows = pl.ds(pl.multiple_of(ch * CH + u * SUB, SUB), SUB)
            here = slice(u * SUB, (u + 1) * SUB)
            metric = met[rows]
            r = resp[rows]
            for p in range(2):
                s = src[p, rows]
                residual = s - r * dn[p, rows]
                earlier = s - r * db[p, rows]
                newest = (residual - earlier).astype(BF16)
                hn[0, p, rows] = newest
                x[p, here] = newest
                x[p, CH + u * SUB : CH + (u + 1) * SUB] = residual.astype(BF16)
                sq[...] += metric * residual * residual
                for i in range(HIST):
                    value = (hr[i, p, rows] if i < HIST - 1 else newest).astype(F32)
                    w[p, i * CH + u * SUB : i * CH + (u + 1) * SUB] = (metric * value).astype(BF16)

    def multiply(ch, w, x):
        rows = pl.ds(pl.multiple_of(ch * CH, CH), CH)
        for p in range(2):
            pairs = [hr[:, p, rows].reshape(7 * CH, NZ), x[p]]
            acc[p] = acc[p] + nt_dot(jnp.concatenate(pairs, axis=0), w[p])

    weigh(0, w0, x0)

    def first(i, carry):
        weigh(2 * i + 1, w1, x1)
        multiply(2 * i, w0, x0)
        weigh(2 * i + 2, w0, x0)
        multiply(2 * i + 1, w1, x1)
        return carry

    lax.fori_loop(0, N_CH // 2 - 1, first, 0)
    late.start()
    for copy in table:
        copy.start()
    weigh(N_CH - 1, w1, x1)
    multiply(N_CH - 2, w0, x0)
    multiply(N_CH - 1, w1, x1)

    def fold3(rows):
        return rows[:, :256] + rows[:, 256:512] + rows[:, 512:]

    def group_sums(lanes):
        l = lax.broadcasted_iota(jnp.int32, (lanes, 128), 0)
        j = lax.broadcasted_iota(jnp.int32, (lanes, 128), 1)
        return jnp.where(l // CH == j, 1.0, 0.0).astype(F32)

    def diagonal(total):
        r = lax.broadcasted_iota(jnp.int32, total.shape, 0)
        l = lax.broadcasted_iota(jnp.int32, total.shape, 1)
        kept = jnp.where(r % CH == l % CH, total, 0.0)
        return jnp.sum(kept.reshape(total.shape[0] // CH, CH, total.shape[1]), axis=1)

    def pack(groups):
        ones = group_sums(groups)
        both = lax.dot_general(
            fold[:, :groups], ones, (((1,), (0,)), ((), ())),
            precision=lax.Precision.HIGHEST, preferred_element_type=F32,
        )
        upper = pltpu.roll(both[:8], 0, 1, stride=8, stride_axis=0)
        lower = pltpu.roll(both[8:], 64, 1, stride=8, stride_axis=0)
        return jnp.sum(upper + lower, axis=0, keepdims=True)

    def spread(slot, row, got, place, peers):
        pay[slot] = row
        got[slot, pl.ds(place, 1)] = row.reshape(1, 1, 128)
        for peer in peers:
            pltpu.make_async_remote_copy(
                src_ref=pay.at[slot],
                dst_ref=got.at[slot, place],
                send_sem=rsend_sem.at[slot],
                recv_sem=rrecv_sem.at[slot],
                device_id=peer,
                device_id_type=MESH,
            ).start()

    def gathered(slot, got, peers):
        sent = got.at[slot, 0 : len(peers)]
        pltpu.make_async_copy(sent, sent, rsend_sem.at[slot]).wait()
        pltpu.make_async_copy(sent, sent, rrecv_sem.at[slot]).wait()
        rows = got[slot].reshape(len(peers) + 1, 128)
        return jnp.sum(rows, axis=0, keepdims=True)

    def unpack(row):
        same = jnp.broadcast_to(row, (8, 128))
        out = same
        for i in range(1, 8):
            out = jnp.where(row128 == i, pltpu.roll(same, 128 - 8 * i, 1), out)
        return out

    def lanes_sum(row, start):
        lanes = lax.broadcasted_iota(jnp.int32, (1, 128), 1)
        kept = jnp.where((lanes >= start) & (lanes < start + 8), row, 0.0)
        return jnp.sum(kept, axis=1, keepdims=True)

    def flip(matrix):
        out = jnp.zeros((8, 128), F32)
        for j in range(8):
            row = jnp.broadcast_to(matrix[j : j + 1], (8, 128))
            column = jnp.sum(jnp.where(row128 == lane128, row, 0.0), axis=1, keepdims=True)
            out = jnp.where(lane128 == j, column, out)
        return out

    def solve(matrix, right):
        m = jnp.where(lane128 < 8, matrix, jnp.where(lane128 == 8, right, 0.0))
        for k in range(8):
            column = jnp.broadcast_to(m[:, k : k + 1], (8, 128))
            row = m[k : k + 1] / column[k : k + 1]
            m = jnp.where(row128 == k, row, m - column * row)
        answer = jnp.broadcast_to(m[:, 8:9], (8, 128))
        for j in range(8):
            cvec[j] = jnp.broadcast_to(answer[j : j + 1], (8, 128))

    fold[...] = jnp.zeros_like(fold)
    fold[0:9] = diagonal(acc[0]) + diagonal(acc[1])
    fold[9:10] = fold3(jnp.sum(sq[...], axis=0, keepdims=True))
    fold[10:11] = fold3(jnp.sum(weights[...], axis=0, keepdims=True))
    row = pack(256)
    pl.semaphore_wait(barrier, len(others_all))
    spread(0, row, gota, col * N_GRP + grp, others_all)

    def prepare(i, carry):
        rows = pl.ds(pl.multiple_of(i * SUB, SUB), SUB)
        inside = met[rows] > 0.0
        precond = jnp.where(inside, pre[rows], 0.0)
        for p in range(2):
            density = dn[p, rows]
            residual = src[p, rows] - resp[rows] * density
            base[p, rows] = jnp.where(inside, density, 0.0) + precond * residual
            for j in range(HIST):
                if j < HIST - 1:
                    drho = hd[j, p, rows].astype(F32)
                else:
                    drho = (density - db[p, rows]).astype(BF16).astype(F32)
                dres = (hr[j, p, rows] if j < HIST - 1 else hn[0, p, rows]).astype(F32)
                step[j, p, rows] = jnp.where(inside, drho, 0.0) + precond * dres
        return carry

    late.wait()
    lax.fori_loop(0, COLS // SUB, prepare, 0)
    for copy in table:
        copy.wait()
    row = gathered(0, gota, others_all)
    margin = unpack(row)
    margin = 0.5 * (margin + flip(margin))
    amat[...] = jnp.where(lane128 < 8, margin, 0.0)
    lanes8 = jnp.broadcast_to(pltpu.roll(row, 64, 1), (8, 128))
    right = jnp.sum(jnp.where(row128 == lane128, lanes8, 0.0), axis=1, keepdims=True)
    weight_total = lanes_sum(row, 80)
    norm0 = jnp.sqrt(lanes_sum(row, 72) / weight_total)
    solve(amat[...], right)

    def mix(t, h, new):
        def go(i, carry):
            local = pl.multiple_of(i * SUB, SUB)
            rows = pl.ds(pl.multiple_of(h * HALF + i * SUB, SUB), SUB)
            coefficient = []
            for j in range(HIST):
                lanes = jnp.concatenate([cvec[j]] * (NZ // 128), axis=1)
                coefficient.append(jnp.concatenate([lanes] * (SUB // 8), axis=0))
            values = []
            for p in range(2):
                mixed = base[p, rows]
                for j in range(HIST):
                    mixed = mixed - coefficient[j] * step[t + j, p, rows]
                new[p, rows] = mixed
                values.append(mixed * SCALE)
            re, im = values[0].astype(BF16), values[1].astype(BF16)
            rmat[h, 0, pl.ds(local, SUB)] = re
            rmat[h, 0, pl.ds(HALF + local, SUB)] = im
            rmat[h, 1, pl.ds(local, SUB)] = im
            rmat[h, 1, pl.ds(HALF + local, SUB)] = (-values[0]).astype(BF16)
            return carry

        lax.fori_loop(0, HALF // SUB, go, 0)

    def transform(t, h, low, high):
        planes = nt_dot(tab[low:high, :NZ], rmat[h, 0]) - nt_dot(tab[low:high, NZ:], rmat[h, 1])
        for p in range(2):
            part = planes[:, p * HALF : (p + 1) * HALF]
            if t == 0:
                prod[h, p, low:high] = part
            else:
                whole[p, low:high, h * HALF : (h + 1) * HALF] = part

    def out_block(t, h):
        start, size = (col * COLS, COLS) if h is None else (col * COLS + h * HALF, HALF)
        return slab_o.at[t, :, :, pl.ds(pl.multiple_of(start, HALF), size)]

    def block(h, dy, dz, dc):
        start = place[dy] * 8 * ZB + (zs[dz] + cs[dc]) * ZB
        planes = whole if h is None else prod.at[h]
        return planes.at[:, pl.ds(pl.multiple_of(start, 8), ZB)]

    def own(t, h):
        return pltpu.make_async_copy(block(h, 0, 0, 0), out_block(t, h), own_sem)

    def send(t, h, pairs):
        for dy, dz in pairs:
            for dc in (1, 0):
                if dy or dz or dc:
                    pltpu.make_async_remote_copy(
                        src_ref=block(h, dy, dz, dc),
                        dst_ref=out_block(t, h),
                        send_sem=send_sem.at[t],
                        recv_sem=recv_sem.at[t],
                        device_id=(ys[dy] + zs[dz] + cs[dc], grp),
                        device_id_type=MESH,
                    ).start()
                else:
                    own(t, h).start()

    def finish(t):
        for h in (0, 1) if t == 0 else (None,):
            own(t, h).wait()
        rows = (N_COL - 1) * COLS
        blocks = slab_o.at[t, :, :, 0:rows]
        pltpu.make_async_copy(blocks, blocks, send_sem.at[t]).wait()
        pltpu.make_async_copy(blocks, blocks, recv_sem.at[t]).wait()

    mix(0, 0, d1)
    transform(0, 0, 0, NZ // 2)
    send(0, 0, near)
    transform(0, 0, NZ // 2, NZ)
    send(0, 0, far[:3])
    mix(0, 1, d1)

    sq[...] = jnp.zeros_like(sq)

    def second(i, carry):
        rows = pl.ds(pl.multiple_of(i * SUB, SUB), SUB)
        metric = met[rows]
        r = resp[rows]
        for p in range(2):
            s = src[p, rows]
            residual = s - r * d1[p, rows]
            earlier = s - r * dn[p, rows]
            newest = (residual - earlier).astype(BF16)
            hn[1, p, rows] = newest
            sq[...] += metric * residual * residual
            half = residual.astype(BF16).astype(F32)
            w2[p, 0, rows] = (metric * newest.astype(F32)).astype(BF16)
            w2[p, 1, rows] = (metric * half).astype(BF16)
        return carry

    def products():
        totals = [jnp.zeros((8 * CH, 2 * CH), F32)] * 2
        for ch in range(N_CH):
            rows = slice(ch * CH, (ch + 1) * CH)
            for p in range(2):
                pairs = [hr[1:7, p, rows].reshape(6 * CH, NZ), hn[0, p, rows], hn[1, p, rows]]
                totals[p] = totals[p] + nt_dot(
                    jnp.concatenate(pairs, axis=0), w2[p, :, rows].reshape(2 * CH, NZ)
                )
        return diagonal(totals[0]) + diagonal(totals[1])

    lax.fori_loop(0, COLS // SUB, second, 0)
    total = products()
    fold[...] = jnp.zeros_like(fold)
    fold[0:8, 0 : 2 * CH] = total
    squares = fold3(jnp.sum(sq[...], axis=0, keepdims=True))
    fold[8:9, 0:128] = squares[:, :128] + squares[:, 128:]
    row = pack(128)
    spread(1, row, gota, col * N_GRP + grp, others_all)
    send(0, 0, far[3:])

    def renew(i, carry):
        rows = pl.ds(pl.multiple_of(i * SUB, SUB), SUB)
        inside = met[rows] > 0.0
        precond = jnp.where(inside, pre[rows], 0.0)
        for p in range(2):
            density = d1[p, rows]
            residual = src[p, rows] - resp[rows] * density
            base[p, rows] = jnp.where(inside, density, 0.0) + precond * residual
            drho = (density - dn[p, rows]).astype(BF16).astype(F32)
            dres = hn[1, p, rows].astype(F32)
            step[HIST, p, rows] = jnp.where(inside, drho, 0.0) + precond * dres
        return carry

    lax.fori_loop(0, COLS // SUB, renew, 0)
    transform(0, 1, 0, NZ)
    send(0, 1, near + far)
    row = gathered(1, gota, others_all)
    table1 = unpack(row)
    newest = table1[:, 0:1]
    across = jnp.sum(jnp.where(row128 == lane128, newest, 0.0), axis=0, keepdims=True)
    shifted = pltpu.roll(pltpu.roll(amat[...], 7, 0), 127, 1)
    matrix = jnp.where(lane128 == 7, newest, jnp.where(row128 == 7, across, shifted))
    norm1 = jnp.sqrt(lanes_sum(row, 64) / weight_total)
    solve(matrix, table1[:, 1:2])

    for h in range(2):
        mix(1, h, mix_o)
        transform(1, h, 0, NZ)
    send(1, None, last)
    lanes = lax.broadcasted_iota(jnp.int32, (1, 128), 1)
    norm_o[...] = jnp.where(lanes == 0, norm0, jnp.where(lanes == 1, norm1, 0.0))
    finish(0)
    finish(1)


def deliver(slab_v, mix_v, norm_v, slab_o, mix_o, norm_o, norm_s, sem):
    copies = []
    for p in range(2):
        for t in range(ITERS):
            for z in range(0, ZB, 8):
                at = (t, p, pl.ds(z, 8))
                copies.append((slab_v.at[at], slab_o.at[at]))
        for k in range(0, COLS, COLS // 4):
            at = (p, pl.ds(k, COLS // 4))
            copies.append((mix_v.at[at], mix_o.at[at]))
    copies = [pltpu.make_async_copy(a, b, sem.at[i]) for i, (a, b) in enumerate(copies)]
    for copy in copies:
        copy.start()
    lanes = lax.broadcasted_iota(jnp.int32, (1, 128), 1)
    for t in range(ITERS):
        norm_s[t] = jnp.sum(jnp.where(lanes == t, norm_v[...], 0.0))
    norms = pltpu.make_async_copy(norm_s, norm_o, sem.at[len(copies)])
    norms.start()
    for copy in copies:
        copy.wait()
    norms.wait()


def body(dn, db, src, resp, hd, hr, shell, screening):
    hbm = pl.BlockSpec(memory_space=pltpu.HBM)
    stack = (2, COLS, NZ)
    vmem = pl.BlockSpec(memory_space=pltpu.VMEM)
    slab_shape = (ITERS, 2, ZB, N_COL * COLS)
    parts = pl.pallas_call(
        kernel,
        out_shape=(pltpu.VMEM(slab_shape, F32), pltpu.VMEM(stack, F32), pltpu.VMEM((1, 128), F32)),
        in_specs=[hbm] * 9,
        out_specs=(vmem, vmem, vmem),
        scratch_shapes=[
            pltpu.SMEM((COLS,), jnp.int32),
            pltpu.SMEM((1,), F32),
            pltpu.VMEM(stack, F32),
            pltpu.VMEM(stack, F32),
            pltpu.VMEM(stack, F32),
            pltpu.VMEM((COLS, NZ), F32),
            pltpu.VMEM((7,) + stack, BF16),
            pltpu.VMEM((7,) + stack, BF16),
            pltpu.VMEM((2,) + stack, BF16),
            pltpu.VMEM((NZ, 2 * NZ), BF16),
            pltpu.VMEM(stack, F32),
            pltpu.VMEM((COLS, NZ), F32),
            pltpu.VMEM((COLS, NZ), F32),
            pltpu.VMEM(stack, F32),
            pltpu.VMEM((9,) + stack, F32),
            pltpu.VMEM((2, HIST * CH, NZ), BF16),
            pltpu.VMEM((2, HIST * CH, NZ), BF16),
            pltpu.VMEM((2, 2 * CH, NZ), BF16),
            pltpu.VMEM((2, 2 * CH, NZ), BF16),
            pltpu.VMEM((2, 2, COLS, NZ), BF16),
            pltpu.VMEM((2, 9 * CH, HIST * CH), F32),
            pltpu.VMEM((SUB, NZ), F32),
            pltpu.VMEM((8, NZ), F32),
            pltpu.VMEM((16, 256), F32),
            pltpu.VMEM((8, 128), F32),
            pltpu.VMEM((8, 8, 128), F32),
            pltpu.VMEM((2, 2, COLS, NZ), BF16),
            pltpu.VMEM((2, 2, NZ, HALF), F32),
            pltpu.VMEM((2, NZ, COLS), F32),
            pltpu.VMEM((2, 1, 128), F32),
            pltpu.VMEM((2, N_COL * N_GRP, 1, 128), F32),
            pltpu.SemaphoreType.DMA((2,)),
            pltpu.SemaphoreType.DMA((N_CH,)),
            pltpu.SemaphoreType.DMA,
            pltpu.SemaphoreType.DMA((4,)),
            pltpu.SemaphoreType.DMA,
            pltpu.SemaphoreType.DMA((ITERS,)),
            pltpu.SemaphoreType.DMA((ITERS,)),
            pltpu.SemaphoreType.DMA((2,)),
            pltpu.SemaphoreType.DMA((2,)),
        ],
        compiler_params=pltpu.CompilerParams(
            collective_id=0, has_side_effects=True, vmem_limit_bytes=54 * 1024 * 1024
        ),
        name="mixing",
    )(dn, db, src, resp, hd, hr, shell, screening, plane_table())
    return pl.pallas_call(
        deliver,
        out_shape=(
            jax.ShapeDtypeStruct(slab_shape, F32),
            jax.ShapeDtypeStruct(stack, F32),
            jax.ShapeDtypeStruct((ITERS,), F32),
        ),
        in_specs=[vmem, vmem, vmem],
        out_specs=(hbm, hbm, hbm),
        scratch_shapes=[pltpu.SMEM((ITERS,), F32), pltpu.SemaphoreType.DMA((21,))],
        compiler_params=pltpu.CompilerParams(vmem_limit_bytes=16 * 1024 * 1024),
        name="deliver",
    )(*parts)


def solution(mesh):
    columns = ("col", "grp")
    return jax.shard_map(
        body,
        mesh=mesh,
        in_specs=(
            P(None, columns, None),
            P(None, columns, None),
            P(None, columns, None),
            P(columns, None),
            P(None, None, columns, None),
            P(None, None, columns, None),
            P(columns),
            P(),
        ),
        out_specs=(P(None, None, "col", "grp"), P(None, columns, None), P()),
        check_vma=False,
    )
```
